32 devices in a mesh: seq: 8 (over z, x), feat: 4 (over y, core).
Axes of the slice: x: 2, y: 2, z: 4, core: 2. Of those that a mesh axis runs over, the one named last changes fastest.
Arguments:
- teacher_states: bfloat16 [4, 8192, 3584], P(None, 'seq', 'feat')
- student_states: bfloat16 [8192, 2304], P('seq'), may hold values from -6 to 6
- projection: bfloat16 [4, 2304, 3584], P(None, 'seq', 'feat'), may hold values from -0.125 to 0.125
- layer_pick: int32 [4], replicated, may hold values from 0 to 3, each once
- validity: int32 [8192], P('seq'), may hold values from 0 to 1, as said below
Outputs:
- whitened_error: bfloat16 [4, 8192, 3584], P(None, 'seq', 'feat')
- total_loss: float32 [], replicated
The draws below stay inside these ranges and needn't reach their ends.
Inputs may be any that keep to these rules, and one draw needn't show every extreme that they name: `validity`: the positions form 2 sequences of 4096 positions each; in each sequence a prefix of 1024 positions or more is 1 and the rest is 0.
All inputs are finite; a program needn't handle non-finite values.
Results may differ from the reference program's by a relative error of at most 0.00045.
Values may be sent and summed in bfloat16 or wider, within the bound.
A program may use at most 128 MiB of HBM per device.

```python
import math
import jax
import jax.numpy as jnp
from jax import lax

D = 3584
DS = 2304
LAYERS = 4
SEQS = 2
TOKENS = 8192


def draw_teacher_states(key, part):
    subkeys = jax.random.split(jax.random.fold_in(key, 101), 4)
    column = jnp.exp(jax.random.uniform(subkeys[0], (LAYERS, 1, D), jnp.float32) * math.log(10.0))
    offset = jax.random.normal(subkeys[1], (LAYERS, 1, D), jnp.float32) * 2.0
    position = jnp.arange(TOKENS, dtype=jnp.float32) / TOKENS
    jitter = jax.random.uniform(subkeys[2], (1, TOKENS, 1), jnp.float32, -0.3, 0.3)
    fluctuation = jax.random.normal(subkeys[3], (LAYERS, TOKENS, D), jnp.float32)
    row_scale = (1.0 + 2.0 * position)[None, :, None] * jnp.exp(jitter)
    return (column * (offset + row_scale * fluctuation)).astype(jnp.bfloat16)


def draw_validity(key, part):
    seq_length = TOKENS // SEQS
    lengths = jax.random.randint(jax.random.fold_in(key, 23), (SEQS,), seq_length // 4, seq_length + 1)
    position = jnp.arange(TOKENS, dtype=jnp.int32) % seq_length
    limits = jnp.repeat(lengths, seq_length)
    return (position < limits).astype(jnp.int32)


def block_levels(key, extent, shards, smallest, high):
    def one(axis_at, parts):
        heights = jax.random.uniform(jax.random.fold_in(jax.random.fold_in(key, 6), axis_at), (parts,), jnp.float32, smallest / len(shards), high / len(shards))
        return jnp.repeat(jnp.exp(heights), extent[axis_at] // parts).reshape((-1,) + (1,) * (len(extent) - axis_at - 1))

    level = one(*shards[0])
    for cut in shards[1:]:
        level = level * one(*cut)
    return level


def scatter_about(key, extent, width, limit, pieces=(), kind=jnp.bfloat16):
    entries = width * jax.random.normal(key, extent, jnp.float32)
    if pieces:
        entries = entries * block_levels(key, extent, pieces, -0.22, 0.18)
    return jnp.clip(entries, -limit, limit).astype(kind)


def setup_inputs(seed: int = 0) -> dict:
    key_of = jax.random.split(jax.random.key(seed), 6)
    return {
        "teacher_states": draw_teacher_states(jax.random.fold_in(key_of[5], 71), 0),
        "student_states": scatter_about(key_of[1], (TOKENS, DS), 1.0, 6.0, ((0, 8),)),
        "projection": scatter_about(key_of[2], (LAYERS, DS, D), DS ** -0.5, 0.125, ((1, 8), (2, 4))),
        "layer_pick": jax.random.permutation(key_of[3], LAYERS).astype(jnp.int32),
        "validity": draw_validity(jax.random.fold_in(key_of[5], 71), 0),
    }


epsilon = 1e-05

def reference(teacher_states, student_states, projection, layer_pick, validity):
    weighting = validity.astype(jnp.float32)
    counted = jnp.sum(weighting)
    squared_total = jnp.zeros((), jnp.float32)
    errors = []
    for number in range(LAYERS):
        chosen = jnp.take(teacher_states, layer_pick[number], axis=0).astype(jnp.float32)
        average = lax.optimization_barrier(jnp.sum(chosen * weighting[:, None], axis=0)) / counted
        centred = chosen - average
        variance = lax.optimization_barrier(jnp.sum(weighting[:, None] * centred * centred, axis=0)) / counted
        target = centred / jnp.sqrt(variance + epsilon)
        predicted = jnp.dot(student_states, projection[number], preferred_element_type=jnp.float32)
        residual = predicted - target
        errors.append((weighting[:, None] * residual).astype(jnp.bfloat16))
        squared_total = squared_total + jnp.sum(weighting[:, None] * residual * residual)
    total_loss = squared_total / (counted * D * LAYERS)
    return (jnp.stack(errors), total_loss)
```

```python
import functools

import jax
import jax.numpy as jnp
from jax import lax
from jax.experimental import pallas as pl
from jax.experimental.pallas import tpu as pltpu
from jax.sharding import PartitionSpec as P

epsilon = 1e-05
WIDE = 2
F32 = jnp.float32


def plain(teacher_states, student_states, projection, layer_pick, validity, *, feats):
    layers = projection.shape[0]
    width = projection.shape[2] * feats
    weighting = validity.astype(F32)
    chosen = jnp.take(teacher_states, layer_pick, axis=0).astype(F32)
    masked = weighting[None, :, None]
    summed, counted = lax.psum((jnp.sum(chosen * masked, axis=1), jnp.sum(weighting)), "seq")
    centred = chosen - (summed / counted)[:, None, :]
    variance = lax.psum(jnp.sum(masked * centred * centred, axis=1), "seq") / counted
    target = centred / jnp.sqrt(variance + epsilon)[:, None, :]
    predicted = jnp.einsum(
        "tr,lrd->ltd",
        student_states,
        lax.all_gather(projection, "seq", axis=1, tiled=True),
        preferred_element_type=F32,
    )
    residual = predicted - target
    squared_total = lax.psum(jnp.sum(masked * residual * residual), ("seq", "feat"))
    return (masked * residual).astype(jnp.bfloat16), squared_total / (counted * width * layers)


def kernel(
    ndev, feats, tile,
    pick, weight, teacher, student, proj, out, loss,
    W, S, T, O, mine, stats, centre, inv, counted, total,
    load_sem, send_sem, recv_sem, stat_send, stat_recv, out_sem,
):
    layers, rows, cols = proj.shape
    tokens = student.shape[0]
    deep = ndev // WIDE
    half = rows // 2
    me = lax.axis_index("seq")
    z, x = me // WIDE, me % WIDE
    other = 1 - x
    pair = z + 1 - 2 * (z % 2)
    reps = cols // 128

    def piece(block, layer, start=0, size=rows):
        return W.at[layer, pl.ds(pl.multiple_of(block * rows + start, 16), size), :]

    def send(src, dst, to, layer, slot, block, part):
        return pltpu.make_async_remote_copy(
            src_ref=src, dst_ref=dst, send_sem=send_sem.at[layer, slot],
            recv_sem=recv_sem.at[layer, block, part],
            device_id={"seq": to}, device_id_type=pl.DeviceIdType.MESH,
        )

    def landed(block, layer, part, start=0, size=rows):
        ref = piece(block, layer, start, size)
        send(ref, ref, me, layer, 0, block, part).wait_recv()

    up, down, across = me + WIDE, me - WIDE, z * WIDE + other
    has_up, has_down = z + 1 < deep, z > 0

    def own(layer, act):
        for slot, to, ok in ((2, across, None), (0, up, has_up), (1, down, has_down)):
            def go(slot=slot, to=to):
                act(send(proj.at[layer], piece(me, layer), to, layer, slot, me, 0))
            go() if ok is None else pl.when(ok)(go)

    def forward(layer, d, act, arrive):
        for sign, to, onward in ((-1, up, has_up), (1, down, has_down)):
            b = z + sign * d
            @pl.when((b >= 0) & (b < deep))
            def _():
                block = b * WIDE + x
                if arrive:
                    landed(block, layer, 0)
                @pl.when(onward)
                def _():
                    ref = piece(block, layer)
                    act(send(ref, ref, to, layer, 3 + b, block, 0))
                @pl.when(b == pair)
                def _():
                    ref = piece(block, layer, 0, half)
                    act(send(ref, ref, across, layer, 3 + deep + b, block, 0))
                @pl.when(b != pair)
                def _():
                    ref = piece(block, layer)
                    act(send(ref, ref, across, layer, 3 + deep + b, block, 0))

    def halves(layer, act, arrive):
        if arrive:
            landed(across, layer, 0)
        ref = piece(across, layer, half, half)
        act(send(ref, ref, pair * WIDE + x, layer, 3 + 2 * deep, across, 1))

    start = lambda c: c.start()
    finish = lambda c: c.wait_send()

    own(0, start)
    own(1, start)
    get_t = pltpu.make_async_copy(teacher, T, load_sem.at[0])
    get_s = pltpu.make_async_copy(student, S, load_sem.at[1])
    get_p = pltpu.make_async_copy(
        proj, W.at[:, pl.ds(pl.multiple_of(me * rows, 16), rows), :], load_sem.at[2]
    )
    get_t.start()
    get_s.start()
    get_p.start()

    chunk = 64
    steps = tokens // chunk

    def spread(at, size):
        w = weight[pl.ds(pl.multiple_of(at, 8), size), :]
        return jnp.concatenate([w] * reps, axis=1)

    def fold(v):
        return jnp.sum(v.reshape(v.shape[0] // 8, 8, cols), axis=0)

    zero = jnp.zeros((8, cols), F32)
    count = jnp.sum(
        lax.fori_loop(
            0, steps,
            lambda i, a: a + jnp.sum(weight[pl.ds(pl.multiple_of(i * chunk, 8), chunk), :].reshape(chunk // 8, 8, 128), axis=0),
            jnp.zeros((8, 128), F32),
        ), axis=0, keepdims=True)
    counts = jnp.concatenate([count] * reps, axis=1)
    get_t.wait()
    means, spreads = [], []
    for s in range(layers):
        def add(i, a):
            c = T[s, pl.ds(pl.multiple_of(i * chunk, 16), chunk), :].astype(F32)
            return a + fold(c * spread(i * chunk, chunk))
        average = jnp.sum(lax.fori_loop(0, steps, add, zero), axis=0, keepdims=True) / jnp.maximum(counts, 1.0)

        def square(i, a):
            c = T[s, pl.ds(pl.multiple_of(i * chunk, 16), chunk), :].astype(F32) - average
            return a + fold(c * c * spread(i * chunk, chunk))
        squares = jnp.sum(lax.fori_loop(0, steps, square, zero), axis=0, keepdims=True)
        means.append(average)
        spreads.append(squares)
    mine[:, :cols] = jnp.concatenate(means + spreads, axis=0)
    mine[:, cols:] = jnp.broadcast_to(count, (2 * layers, 128))

    def stat(k):
        return pltpu.make_async_remote_copy(
            src_ref=mine, dst_ref=stats.at[k], send_sem=stat_send.at[k], recv_sem=stat_recv.at[k],
            device_id={"seq": (me + k) % ndev}, device_id_type=pl.DeviceIdType.MESH,
        )

    for k in range(1, ndev):
        stat(k).start()
    stats[0] = mine[...]
    total[...] = jnp.zeros_like(total)

    def combine():
        for k in range(1, ndev):
            stat(k).wait_recv()
        held = [stats[k] for k in range(ndev)]
        weights = [jnp.concatenate([v[0:1, cols:]] * reps, axis=1) for v in held]
        n = sum(weights[1:], weights[0])
        counted[...] = jnp.broadcast_to(n, (8, cols))
        for s in range(layers):
            average = jnp.zeros((1, cols), F32)
            for nk, v in zip(weights, held):
                average = average + nk * v[s : s + 1, :cols]
            average = average / n
            squares = jnp.zeros((1, cols), F32)
            for nk, v in zip(weights, held):
                off = v[s : s + 1, :cols] - average
                squares = squares + v[layers + s : layers + s + 1, :cols] + nk * off * off
            centre[s] = jnp.broadcast_to(average, (8, cols))
            inv[s] = jnp.broadcast_to(1.0 / jnp.sqrt(squares / n + epsilon), (8, cols))

    def write(layer, m):
        at = pl.ds(pl.multiple_of(m * tile, 16), tile)
        return pltpu.make_async_copy(O.at[layer, at, :], out.at[layer, at, :], out_sem.at[layer, m])

    def compute(layer):
        for b in range(deep):
            block = b * WIDE + other
            @pl.when((b != z) & (b != pair))
            def _():
                landed(block, layer, 0)
        block = pair * WIDE + other
        landed(block, layer, 0, 0, half)
        landed(block, layer, 1, half, half)
        which = pick[layer]
        average = centre[which][0:1]
        inverse = inv[which][0:1]

        def body(m, c):
            at = pl.ds(pl.multiple_of(m * tile, 16), tile)
            predicted = jnp.dot(S[at, :], W[layer], preferred_element_type=F32)
            target = (T[which, at, :].astype(F32) - average) * inverse
            residual = predicted - target
            w = spread(m * tile, tile) * residual
            O[layer, at, :] = w.astype(O.dtype)
            total[...] += fold(w * residual)
            write(layer, m).start()
            return c
        lax.fori_loop(0, tokens // tile, body, 0)

    def phase(p, c):
        @pl.when(p < layers)
        def _():
            for d in range(1, deep):
                forward(p, d, start, True)
        @pl.when(p + 2 < layers)
        def _():
            own(p + 2, start)
            halves(p, start, True)
        @pl.when(p == layers - 1)
        def _():
            halves(layers - 2, start, True)
            halves(layers - 1, start, True)
        @pl.when(p == 1)
        def _():
            combine()
            get_s.wait()
            get_p.wait()
        @pl.when(p > 0)
        def _():
            compute(p - 1)
        return c
    lax.fori_loop(0, layers + 1, phase, 0)

    loss[0, 0] = jnp.sum(total[...] / (counted[...] * F32(cols * feats * layers)))

    def drain(layer, c):
        own(layer, finish)
        for d in range(1, deep):
            forward(layer, d, finish, False)
        halves(layer, finish, False)
        for m in range(tokens // tile):
            write(layer, m).wait()
        return c
    lax.fori_loop(0, layers, drain, 0)
    for k in range(1, ndev):
        stat(k).wait_send()


def fused(teacher_states, student_states, projection, layer_pick, validity, *, ndev, feats, tile):
    layers, rows, cols = projection.shape
    tokens, depth = student_states.shape
    deep = ndev // WIDE
    weight = jnp.broadcast_to(validity.astype(F32)[:, None], (tokens, 128))
    anywhere = pl.BlockSpec(memory_space=pl.ANY)
    smem = pl.BlockSpec(memory_space=pltpu.SMEM)
    bf16 = jnp.bfloat16
    error, partial = pl.pallas_call(
        functools.partial(kernel, ndev, feats, tile),
        out_shape=(
            jax.ShapeDtypeStruct((layers, tokens, cols), bf16),
            jax.ShapeDtypeStruct((1, 1), F32),
        ),
        in_specs=[smem, pl.BlockSpec(memory_space=pltpu.VMEM), anywhere, anywhere, anywhere],
        out_specs=(anywhere, smem),
        scratch_shapes=[
            pltpu.VMEM((layers, rows * ndev, cols), bf16),
            pltpu.VMEM((tokens, depth), bf16),
            pltpu.VMEM((layers, tokens, cols), bf16),
            pltpu.VMEM((layers, tokens, cols), bf16),
            pltpu.VMEM((2 * layers, cols + 128), F32),
            pltpu.VMEM((ndev, 2 * layers, cols + 128), F32),
            pltpu.VMEM((layers, 8, cols), F32),
            pltpu.VMEM((layers, 8, cols), F32),
            pltpu.VMEM((8, cols), F32),
            pltpu.VMEM((8, cols), F32),
            pltpu.SemaphoreType.DMA((3,)),
            pltpu.SemaphoreType.DMA((layers, 4 + 2 * deep)),
            pltpu.SemaphoreType.DMA((layers, ndev, 2)),
            pltpu.SemaphoreType.DMA((ndev,)),
            pltpu.SemaphoreType.DMA((ndev,)),
            pltpu.SemaphoreType.DMA((layers, tokens // tile)),
        ],
        compiler_params=pltpu.CompilerParams(
            has_side_effects=True, vmem_limit_bytes=67043328
        ),
        name="gather_whiten",
    )(layer_pick, weight, teacher_states, student_states, projection)
    return error, lax.psum(partial[0, 0], ("seq", "feat"))


def solution(mesh):
    ndev, feats = mesh.shape["seq"], mesh.shape["feat"]
    tile = 256
    placed = (P(None, "seq", "feat"), P("seq", None), P(None, "seq", "feat"), P(), P("seq"))

    def step(teacher_states, student_states, projection, layer_pick, validity):
        layers, rows, cols = projection.shape
        tokens = student_states.shape[0]
        kept = 2 * (rows * ndev * cols * layers + tokens * rows * ndev + 2 * layers * tokens * cols)
        fits = kept < (48 << 20) and ndev % (2 * WIDE) == 0 and layers >= 2
        if fits and rows % 32 == 0 and cols % 128 == 0 and tokens % tile == 0:
            run = functools.partial(fused, ndev=ndev, feats=feats, tile=tile)
        else:
            run = functools.partial(plain, feats=feats)
        return run(teacher_states, student_states, projection, layer_pick, validity)

    return jax.shard_map(
        step, mesh=mesh, in_specs=placed, out_specs=(P(None, "seq", "feat"), P()), check_vma=False
    )
```

```python
import functools

import jax
import jax.numpy as jnp
from jax import lax
from jax.experimental import pallas as pl
from jax.experimental.pallas import tpu as pltpu
from jax.sharding import PartitionSpec as P

epsilon = 1e-05
WIDE = 2
F32 = jnp.float32


def plain(teacher_states, student_states, projection, layer_pick, validity, *, feats):
    layers = projection.shape[0]
    width = projection.shape[2] * feats
    weighting = validity.astype(F32)
    chosen = jnp.take(teacher_states, layer_pick, axis=0).astype(F32)
    masked = weighting[None, :, None]
    summed, counted = lax.psum((jnp.sum(chosen * masked, axis=1), jnp.sum(weighting)), "seq")
    centred = chosen - (summed / counted)[:, None, :]
    variance = lax.psum(jnp.sum(masked * centred * centred, axis=1), "seq") / counted
    target = centred / jnp.sqrt(variance + epsilon)[:, None, :]
    predicted = jnp.einsum(
        "tr,lrd->ltd",
        student_states,
        lax.all_gather(projection, "seq", axis=1, tiled=True),
        preferred_element_type=F32,
    )
    residual = predicted - target
    squared_total = lax.psum(jnp.sum(masked * residual * residual), ("seq", "feat"))
    return (masked * residual).astype(jnp.bfloat16), squared_total / (counted * width * layers)


def kernel(
    ndev, feats, tile,
    pick, weight, teacher, student, proj, out, loss,
    W, S, T, O, mine, stats, centre, inv, counted, total, part,
    load_sem, send_sem, recv_sem, stat_send, stat_recv, part_send, part_recv, out_sem,
):
    layers, rows, cols = proj.shape
    tokens = student.shape[0]
    deep = ndev // WIDE
    half = rows // 2
    me = lax.axis_index("seq")
    z, x = me // WIDE, me % WIDE
    other = 1 - x
    pair = z + 1 - 2 * (z % 2)
    reps = cols // 128

    def piece(block, layer, start=0, size=rows):
        return W.at[layer, pl.ds(pl.multiple_of(block * rows + start, 16), size), :]

    def send(src, dst, to, layer, slot, block, part):
        return pltpu.make_async_remote_copy(
            src_ref=src, dst_ref=dst, send_sem=send_sem.at[layer, slot],
            recv_sem=recv_sem.at[layer, block, part],
            device_id={"seq": to}, device_id_type=pl.DeviceIdType.MESH,
        )

    def landed(block, layer, part, start=0, size=rows):
        ref = piece(block, layer, start, size)
        send(ref, ref, me, layer, 0, block, part).wait_recv()

    up, down, across = me + WIDE, me - WIDE, z * WIDE + other
    has_up, has_down = z + 1 < deep, z > 0

    def own(layer, act):
        for slot, to, ok in ((2, across, None), (0, up, has_up), (1, down, has_down)):
            def go(slot=slot, to=to):
                act(send(proj.at[layer], piece(me, layer), to, layer, slot, me, 0))
            go() if ok is None else pl.when(ok)(go)

    def forward(layer, d, act, arrive):
        for sign, to, onward in ((-1, up, has_up), (1, down, has_down)):
            b = z + sign * d
            @pl.when((b >= 0) & (b < deep))
            def _():
                block = b * WIDE + x
                if arrive:
                    landed(block, layer, 0)
                @pl.when(onward)
                def _():
                    ref = piece(block, layer)
                    act(send(ref, ref, to, layer, 3 + b, block, 0))
                @pl.when(b == pair)
                def _():
                    ref = piece(block, layer, 0, half)
                    act(send(ref, ref, across, layer, 3 + deep + b, block, 0))
                @pl.when(b != pair)
                def _():
                    ref = piece(block, layer)
                    act(send(ref, ref, across, layer, 3 + deep + b, block, 0))

    def halves(layer, act, arrive):
        if arrive:
            landed(across, layer, 0)
        ref = piece(across, layer, half, half)
        act(send(ref, ref, pair * WIDE + x, layer, 3 + 2 * deep, across, 1))

    start = lambda c: c.start()
    finish = lambda c: c.wait_send()

    for l in range(layers):
        own(l, start)
    get_t = pltpu.make_async_copy(teacher, T, load_sem.at[0])
    get_s = pltpu.make_async_copy(student, S, load_sem.at[1])
    get_p = pltpu.make_async_copy(
        proj, W.at[:, pl.ds(pl.multiple_of(me * rows, 16), rows), :], load_sem.at[2]
    )
    get_t.start()
    get_s.start()
    get_p.start()

    chunk = 64
    steps = tokens // chunk

    def spread(at, size):
        w = weight[pl.ds(pl.multiple_of(at, 8), size), :]
        return jnp.concatenate([w] * reps, axis=1)

    def fold(v):
        return jnp.sum(v.reshape(v.shape[0] // 8, 8, cols), axis=0)

    zero = jnp.zeros((8, cols), F32)
    count = jnp.sum(
        lax.fori_loop(
            0, steps,
            lambda i, a: a + jnp.sum(weight[pl.ds(pl.multiple_of(i * chunk, 8), chunk), :].reshape(chunk // 8, 8, 128), axis=0),
            jnp.zeros((8, 128), F32),
        ), axis=0, keepdims=True)
    counts = jnp.concatenate([count] * reps, axis=1)
    get_t.wait()
    means, spreads = [], []
    for s in range(layers):
        def add(i, a):
            c = T[s, pl.ds(pl.multiple_of(i * chunk, 16), chunk), :].astype(F32)
            return a + fold(c * spread(i * chunk, chunk))
        average = jnp.sum(lax.fori_loop(0, steps, add, zero), axis=0, keepdims=True) / jnp.maximum(counts, 1.0)

        def square(i, a):
            c = T[s, pl.ds(pl.multiple_of(i * chunk, 16), chunk), :].astype(F32) - average
            return a + fold(c * c * spread(i * chunk, chunk))
        squares = jnp.sum(lax.fori_loop(0, steps, square, zero), axis=0, keepdims=True)
        means.append(average)
        spreads.append(squares)
    mine[:, :cols] = jnp.concatenate(means + spreads, axis=0)
    mine[:, cols:] = jnp.broadcast_to(count, (2 * layers, 128))

    def stat(k):
        return pltpu.make_async_remote_copy(
            src_ref=mine, dst_ref=stats.at[k], send_sem=stat_send.at[k], recv_sem=stat_recv.at[k],
            device_id={"seq": (me + k) % ndev}, device_id_type=pl.DeviceIdType.MESH,
        )

    for k in range(1, ndev):
        stat(k).start()
    stats[0] = mine[...]
    total[...] = jnp.zeros_like(total)

    def combine():
        for k in range(1, ndev):
            stat(k).wait_recv()
        held = [stats[k] for k in range(ndev)]
        weights = [jnp.concatenate([v[0:1, cols:]] * reps, axis=1) for v in held]
        n = sum(weights[1:], weights[0])
        counted[...] = jnp.broadcast_to(n, (8, cols))
        for s in range(layers):
            average = jnp.zeros((1, cols), F32)
            for nk, v in zip(weights, held):
                average = average + nk * v[s : s + 1, :cols]
            average = average / n
            squares = jnp.zeros((1, cols), F32)
            for nk, v in zip(weights, held):
                off = v[s : s + 1, :cols] - average
                squares = squares + v[layers + s : layers + s + 1, :cols] + nk * off * off
            centre[s] = jnp.broadcast_to(average, (8, cols))
            inv[s] = jnp.broadcast_to(1.0 / jnp.sqrt(squares / n + epsilon), (8, cols))

    def write(layer, m):
        at = pl.ds(pl.multiple_of(m * tile, 16), tile)
        return pltpu.make_async_copy(O.at[layer, at, :], out.at[layer, at, :], out_sem.at[layer, m])

    def compute(layer):
        for b in range(deep):
            block = b * WIDE + other
            @pl.when((b != z) & (b != pair))
            def _():
                landed(block, layer, 0)
        block = pair * WIDE + other
        landed(block, layer, 0, 0, half)
        landed(block, layer, 1, half, half)
        which = pick[layer]
        average = centre[which][0:1]
        inverse = inv[which][0:1]

        def body(m, c):
            at = pl.ds(pl.multiple_of(m * tile, 16), tile)
            predicted = jnp.dot(S[at, :], W[layer], preferred_element_type=F32)
            target = (T[which, at, :].astype(F32) - average) * inverse
            residual = predicted - target
            w = spread(m * tile, tile) * residual
            O[layer, at, :] = w.astype(O.dtype)
            total[...] += fold(w * residual)
            write(layer, m).start()
            return c
        lax.fori_loop(0, tokens // tile, body, 0)

    last = deep - 1
    for d in range(1, last):
        def near(l, c, d=d):
            forward(l, d, start, True)
            if d == last - 1:
                @pl.when(l < layers - 2)
                def _():
                    halves(l, start, True)
                @pl.when(l == layers - 1)
                def _():
                    halves(layers - 2, start, True)
                    halves(layers - 1, start, True)
            return c
        lax.fori_loop(0, layers, near, 0)
    combine()
    get_s.wait()
    get_p.wait()

    def phase(p, c):
        @pl.when(p < layers)
        def _():
            forward(p, last, start, True)
        @pl.when(p > 0)
        def _():
            compute(p - 1)
        return c
    lax.fori_loop(0, layers + 1, phase, 0)

    share = total[...] / (counted[...] * F32(cols * feats * layers))
    part[0] = sum(share[:, i * 128 : i * 128 + 128] for i in range(reps))

    def gossip(axis, k, size, index, first):
        return pltpu.make_async_remote_copy(
            src_ref=part.at[first], dst_ref=part.at[first + k],
            send_sem=part_send.at[first + k], recv_sem=part_recv.at[first + k],
            device_id={axis: (index + k) % size}, device_id_type=pl.DeviceIdType.MESH,
        )

    def meet(axis, size, index, first):
        copies = [gossip(axis, k, size, index, first) for k in range(1, size)]
        for c in copies:
            c.start()
        for c in copies:
            c.wait_recv()
        return copies, sum(part[first + k] for k in range(size))

    sent, value = meet("feat", feats, lax.axis_index("feat"), 0)
    part[feats] = value
    more, value = meet("seq", ndev, me, feats)
    loss[0, 0] = jnp.sum(value)
    for c in sent + more:
        c.wait_send()

    def drain(layer, c):
        own(layer, finish)
        for d in range(1, deep):
            forward(layer, d, finish, False)
        halves(layer, finish, False)
        for m in range(tokens // tile):
            write(layer, m).wait()
        return c
    lax.fori_loop(0, layers, drain, 0)
    for k in range(1, ndev):
        stat(k).wait_send()


def fused(teacher_states, student_states, projection, layer_pick, validity, *, ndev, feats, tile):
    layers, rows, cols = projection.shape
    tokens, depth = student_states.shape
    deep = ndev // WIDE
    weight = jnp.broadcast_to(validity.astype(F32)[:, None], (tokens, 128))
    anywhere = pl.BlockSpec(memory_space=pl.ANY)
    smem = pl.BlockSpec(memory_space=pltpu.SMEM)
    bf16 = jnp.bfloat16
    error, partial = pl.pallas_call(
        functools.partial(kernel, ndev, feats, tile),
        out_shape=(
            jax.ShapeDtypeStruct((layers, tokens, cols), bf16),
            jax.ShapeDtypeStruct((1, 1), F32),
        ),
        in_specs=[smem, pl.BlockSpec(memory_space=pltpu.VMEM), anywhere, anywhere, anywhere],
        out_specs=(anywhere, smem),
        scratch_shapes=[
            pltpu.VMEM((layers, rows * ndev, cols), bf16),
            pltpu.VMEM((tokens, depth), bf16),
            pltpu.VMEM((layers, tokens, cols), bf16),
            pltpu.VMEM((layers, tokens, cols), bf16),
            pltpu.VMEM((2 * layers, cols + 128), F32),
            pltpu.VMEM((ndev, 2 * layers, cols + 128), F32),
            pltpu.VMEM((layers, 8, cols), F32),
            pltpu.VMEM((layers, 8, cols), F32),
            pltpu.VMEM((8, cols), F32),
            pltpu.VMEM((8, cols), F32),
            pltpu.VMEM((feats + ndev, 8, 128), F32),
            pltpu.SemaphoreType.DMA((3,)),
            pltpu.SemaphoreType.DMA((layers, 4 + 2 * deep)),
            pltpu.SemaphoreType.DMA((layers, ndev, 2)),
            pltpu.SemaphoreType.DMA((ndev,)),
            pltpu.SemaphoreType.DMA((ndev,)),
            pltpu.SemaphoreType.DMA((feats + ndev,)),
            pltpu.SemaphoreType.DMA((feats + ndev,)),
            pltpu.SemaphoreType.DMA((layers, tokens // tile)),
        ],
        compiler_params=pltpu.CompilerParams(
            has_side_effects=True, vmem_limit_bytes=67043328
        ),
        name="gather_whiten",
    )(layer_pick, weight, teacher_states, student_states, projection)
    return error, partial[0, 0]


def solution(mesh):
    ndev, feats = mesh.shape["seq"], mesh.shape["feat"]
    tile = 256
    placed = (P(None, "seq", "feat"), P("seq", None), P(None, "seq", "feat"), P(), P("seq"))

    def step(teacher_states, student_states, projection, layer_pick, validity):
        layers, rows, cols = projection.shape
        tokens = student_states.shape[0]
        kept = 2 * (rows * ndev * cols * layers + tokens * rows * ndev + 2 * layers * tokens * cols)
        fits = kept < (48 << 20) and ndev % (2 * WIDE) == 0 and ndev > 2 * WIDE and layers >= 2
        if fits and rows % 32 == 0 and cols % 128 == 0 and tokens % tile == 0:
            run = functools.partial(fused, ndev=ndev, feats=feats, tile=tile)
        else:
            run = functools.partial(plain, feats=feats)
        return run(teacher_states, student_states, projection, layer_pick, validity)

    return jax.shard_map(
        step, mesh=mesh, in_specs=placed, out_specs=(P(None, "seq", "feat"), P()), check_vma=False
    )
```
